512 devices in a mesh: dp: 32 (over y_hi, z), mp: 16 (over x, y_lo, core).
Axes of the slice: x: 4, y: 4 (y_hi: 2, y_lo: 2; y = y_hi * 2 + y_lo), z: 16, core: 2. Of those that a mesh axis runs over, the one named last changes fastest.
Arguments:
- tokens: bfloat16 [32768, 4096], P('dp', 'mp'), may hold values from -6 to 6
- right_weight: bfloat16 [64, 64, 64], P('mp', 'dp'), may hold values from -0.75 to 0.75
- left_weight: bfloat16 [64, 64, 64], P('mp', 'dp'), may hold values from -0.75 to 0.75
- cotangent: bfloat16 [32768, 4096], P('dp', 'mp'), may hold values from -0.032958984 to 0.032958984
Outputs:
- activated: bfloat16 [32768, 4096], P('dp', 'mp')
- grad_right: float32 [64, 64, 64], P('mp', 'dp')
- grad_left: float32 [64, 64, 64], P('mp', 'dp')
The draws below stay inside these ranges and needn't reach their ends.
All inputs are finite; a program needn't handle non-finite values.
Results may differ from the reference program's by a relative error of at most 0.0056.
Values may be sent and summed in bfloat16 or wider, within the bound.
A program may use at most 64 MiB of HBM per device.

```python
import jax
import jax.numpy as jnp
from jax import lax

NB = 64
BS = 64
TOK_DEV = 1024
D = 4096
TOKENS = 32768
N_DP = 32


def block_scale(rng, dims, cuts, smallest, top_value):
    loudness, own = 1.0, jax.random.fold_in(rng, 6)
    for dim, shards_of in cuts:
        heights = jnp.exp(jax.random.uniform(jax.random.fold_in(own, dim), (shards_of,), jnp.float32, smallest / len(cuts), top_value / len(cuts)))
        loudness = loudness * jnp.repeat(heights, dims[dim] // shards_of).reshape([-1 if axis == dim else 1 for axis in range(len(dims))])
    return loudness


def scatter_about(rng, dims, width, limit, shards=(), dtype=jnp.bfloat16):
    result = width * jax.random.normal(rng, dims, jnp.float32)
    if shards:
        result = result * block_scale(rng, dims, shards, -0.22, 0.18)
    return jnp.clip(result, -limit, limit).astype(dtype)


def setup_inputs(seed: int = 0) -> dict:
    keys = jax.random.split(jax.random.key(seed), 5)
    return {
        "tokens": scatter_about(keys[0], (TOKENS, D), 1.0, 6.0, ((0, 32), (1, 16))),
        "right_weight": scatter_about(keys[1], (NB, BS, BS), BS ** -0.5, 0.75, ((0, 16), (1, 32))),
        "left_weight": scatter_about(keys[2], (BS, NB, BS), NB ** -0.5, 0.75, ((0, 16), (1, 32))),
        "cotangent": scatter_about(keys[3], (TOKENS, D), ((TOK_DEV * N_DP) ** -0.5), 0.032958984, ((0, 32), (1, 16))),
    }


def gelu_slope(pre):
    cdf = 0.5 * (1.0 + lax.erf(pre * 0.7071067811865476))
    density = jnp.exp(-0.5 * pre * pre) * 0.3989422804014327
    return cdf + pre * density


def reference(tokens, right_weight, left_weight, cotangent):
    right_f = right_weight.astype(jnp.float32)
    left_f = left_weight.astype(jnp.float32)
    xs_all = tokens.reshape(N_DP, TOK_DEV, NB, BS)
    gs_all = cotangent.reshape(N_DP, TOK_DEV, BS, BS)

    def step(carry, pieces):
        grad_r, grad_l = carry
        xs, gs = pieces
        xs_f = xs.astype(jnp.float32)
        inner = jnp.einsum('tik,ikm->tim', xs_f, right_f).astype(jnp.bfloat16)
        inner_f = inner.astype(jnp.float32)
        pre = jnp.einsum('tim,min->tmn', inner_f, left_f)
        activated = jax.nn.gelu(pre, approximate=False).astype(jnp.bfloat16)
        dpre = (gs.astype(jnp.float32) * gelu_slope(pre)).astype(jnp.bfloat16)
        dpre_f = dpre.astype(jnp.float32)
        grad_l = grad_l + jnp.einsum('tim,tmn->min', inner_f, dpre_f)
        dinner = jnp.einsum('tmn,min->tim', dpre_f, left_f).astype(jnp.bfloat16)
        grad_r = grad_r + jnp.einsum('tik,tim->ikm', xs_f, dinner.astype(jnp.float32))
        return (grad_r, grad_l), activated

    start = (jnp.zeros((NB, BS, BS), jnp.float32), jnp.zeros((BS, NB, BS), jnp.float32))
    (grad_right, grad_left), outs = lax.scan(step, start, (xs_all, gs_all))
    activated = outs.reshape(N_DP * TOK_DEV, NB * BS)
    return activated, grad_right, grad_left
```

```python
import functools

import jax
import jax.numpy as jnp
from jax import lax
from jax.experimental import pallas as pl
from jax.experimental.pallas import tpu as pltpu
from jax.sharding import PartitionSpec as P

MESH = pl.DeviceIdType.MESH
BF = jnp.bfloat16
F32 = jnp.float32
CHUNK = 256


def iota(dim, shape=(256, 256)):
    return lax.broadcasted_iota(jnp.int32, shape, dim)


def nn(a, b):
    return lax.dot_general(a, b, (((1,), (0,)), ((), ())), preferred_element_type=F32)


def nt(a, b):
    return lax.dot_general(a, b, (((1,), (1,)), ((), ())), preferred_element_type=F32)


def ones_where(cond):
    return jnp.where(cond, 1.0, 0.0).astype(BF)


def diagonal_blocks(full):
    lane = iota(1, (64, 256)) // 64
    total = jnp.zeros((64, 256), F32)
    for b in range(4):
        total = jnp.where(lane == b, full[64 * b : 64 * b + 64], total)
    return total


def kernel(
    n_dp,
    n_mp,
    x_hbm,
    rw_hbm,
    lw_hbm,
    cot_hbm,
    act_hbm,
    gr_ref,
    gl_ref,
    x_v,
    cot_v,
    rw_v,
    lw_v,
    xt_v,
    cott_v,
    s1_v,
    r_v,
    s2_v,
    d_v,
    actt_v,
    act_v,
    send_rw,
    send_lw,
    got_rw,
    got_lw,
    kr_v,
    kl_v,
    got_kr,
    got_kl,
    in_sem,
    out_sem,
    w_send,
    w_recv,
    a_send,
    a_recv,
    g_send,
    g_recv,
):
    tok = x_v.shape[0]
    chunks = tok // CHUNK
    dp = lax.axis_index("dp")
    mp = lax.axis_index("mp")
    n_z = n_dp // 2

    def dp_peer(t):
        o = t // 2
        step = (o + 1) // 2
        zoff = n_z // 2 + jnp.where(o % 2 == 1, -step, step)
        z = lax.rem(lax.rem(dp, n_z) + zoff + n_z, n_z)
        y = lax.rem(dp // n_z + 1 + lax.rem(t, 2), 2)
        return y * n_z + z

    def mp_peer(j):
        return lax.rem(mp + j, n_mp)

    loads = [
        pltpu.make_async_copy(rw_hbm, rw_v, in_sem.at[0]),
        pltpu.make_async_copy(lw_hbm, lw_v, in_sem.at[1]),
        pltpu.make_async_copy(x_hbm, x_v, in_sem.at[2]),
        pltpu.make_async_copy(cot_hbm, cot_v, in_sem.at[3]),
    ]
    for load in loads:
        load.start()

    barrier = pltpu.get_barrier_semaphore()

    @pl.loop(0, n_dp - 1)
    def _(t):
        pl.semaphore_signal(barrier, inc=1, device_id={"dp": dp_peer(t)}, device_id_type=MESH)

    @pl.loop(1, n_mp)
    def _(j):
        pl.semaphore_signal(barrier, inc=1, device_id={"mp": mp_peer(j)}, device_id_type=MESH)

    loads[0].wait()
    loads[1].wait()
    mine_r = jnp.concatenate([rw_v[i].astype(F32) for i in range(4)], axis=1).astype(BF)
    mine_l = jnp.concatenate([lw_v[i].astype(F32) for i in range(4)], axis=1).astype(BF)
    send_rw[...] = mine_r
    send_lw[...] = mine_l
    got_rw[dp] = mine_r
    got_lw[dp] = mine_l

    pl.semaphore_wait(barrier, n_dp - 1 + n_mp - 1)

    for k, (src, dst) in enumerate(((send_rw, got_rw), (send_lw, got_lw))):

        @pl.loop(0, n_dp - 1)
        def _(t):
            pltpu.make_async_remote_copy(
                src_ref=src,
                dst_ref=dst.at[dp],
                send_sem=w_send.at[k],
                recv_sem=w_recv.at[k],
                device_id={"dp": dp_peer(t)},
                device_id_type=MESH,
            ).start()

    loads[2].wait()
    loads[3].wait()
    xt_v[...] = x_v[...].T
    cott_v[...] = cot_v[...].T

    row, col = iota(0), iota(1)
    to_r = ones_where(col == (row % 4) * 64 + row // 4)
    from_r = ones_where(row == (col % 4) * 64 + col // 4)
    rep = ones_where(iota(1, (256, 64)) == (iota(0, (256, 64)) // 16) * 4 + iota(0, (256, 64)) % 4)

    others = got_rw.at[pl.ds(0, n_dp - 1)]
    pltpu.make_async_copy(others, others, w_recv.at[0]).wait()
    rows = got_rw[...].reshape(64, 256).astype(F32)
    lane = iota(1, (64, 256)) // 64
    block_diag = jnp.concatenate([jnp.where(lane == b, rows, 0.0) for b in range(4)], axis=0).astype(BF)
    first = nt(to_r, block_diag).astype(BF)

    def exchange(c, src, dst, k):
        mine = pl.ds(pl.multiple_of(16 * mp, 16), 16)

        @pl.loop(1, n_mp)
        def _(j):
            q = mp_peer(j)
            pltpu.make_async_remote_copy(
                src_ref=src.at[c, pl.ds(pl.multiple_of(16 * q, 16), 16), :],
                dst_ref=dst.at[c, mine, :],
                send_sem=a_send.at[k, c],
                recv_sem=a_recv.at[k, c],
                device_id={"mp": q},
                device_id_type=MESH,
            ).start()

        dst[c, mine, :] = src[c, mine, :]

    def arrived(dst, c, k):
        others = dst.at[c, pl.ds(0, 16 * (n_mp - 1)), :]
        pltpu.make_async_copy(others, others, a_recv.at[k, c]).wait()

    for c in range(chunks):
        s1_v[c] = nn(first, xt_v[:, CHUNK * c : CHUNK * (c + 1)]).astype(BF)
        exchange(c, s1_v, r_v, 0)

    others_l = got_lw.at[pl.ds(0, n_dp - 1)]
    pltpu.make_async_copy(others_l, others_l, w_recv.at[1]).wait()
    spread = nn(rep, got_lw[...].reshape(64, 256))
    second_f = jnp.where(col // 64 == (row // 4) % 4, spread, 0.0)
    second = second_f.astype(BF)
    second_t = second_f.T.astype(BF)

    left = jnp.zeros((256, 256), F32)
    for c in range(chunks):
        arrived(r_v, c, 0)
        inner = r_v[c]
        pre = nn(second_t, inner)
        cdf = 0.5 * (1.0 + lax.erf(pre * 0.7071067811865476))
        density = jnp.exp(-0.5 * pre * pre) * 0.3989422804014327
        cot = cott_v[:, CHUNK * c : CHUNK * (c + 1)].astype(F32)
        dpre = (cot * (cdf + pre * density)).astype(BF)
        s2_v[c] = nn(second, dpre).astype(BF)
        exchange(c, s2_v, d_v, 1)
        actt_v[:, CHUNK * c : CHUNK * (c + 1)] = (pre * cdf).astype(BF)
        left = left + nt(inner, dpre)

    def scatter(src, dst, k):
        @pl.loop(0, n_dp - 1)
        def _(t):
            peer = dp_peer(t)
            pltpu.make_async_remote_copy(
                src_ref=src.at[peer],
                dst_ref=dst.at[dp],
                send_sem=g_send.at[k],
                recv_sem=g_recv.at[k],
                device_id={"dp": peer},
                device_id_type=MESH,
            ).start()

        dst[dp] = src[dp]

    def collect(dst, k):
        others = dst.at[pl.ds(0, n_dp - 1)]
        pltpu.make_async_copy(others, others, g_recv.at[k]).wait()
        return jnp.sum(dst[...], axis=0)

    left = jnp.where(col // 64 == (row // 4) % 4, left, 0.0)
    left = jnp.sum(left.reshape(16, 4, 4, 256), axis=1)
    kl_v[...] = left.reshape(n_dp, 2, 256)
    scatter(kl_v, got_kl, 0)

    right = jnp.zeros((256, 256), F32)
    for c in range(chunks):
        arrived(d_v, c, 1)
        dinner = nn(from_r, d_v[c]).astype(BF)
        right = right + nt(xt_v[:, CHUNK * c : CHUNK * (c + 1)], dinner)
    kr_v[...] = diagonal_blocks(right).reshape(n_dp, 2, 256)
    scatter(kr_v, got_kr, 1)

    act_v[...] = actt_v[...].T
    store = pltpu.make_async_copy(act_v, act_hbm, out_sem)
    store.start()

    sum_l = collect(got_kl, 0)
    for b in range(4):
        gl_ref[b] = sum_l[:, 64 * b : 64 * b + 64]
    sum_r = collect(got_kr, 1)
    for b in range(4):
        gr_ref[b] = sum_r[:, 64 * b : 64 * b + 64]

    for k, dst in enumerate((got_rw, got_lw)):
        sent = dst.at[pl.ds(0, n_dp - 1)]
        pltpu.make_async_copy(sent, sent, w_send.at[k]).wait()
    for k, src in enumerate((s1_v, s2_v)):
        for c in range(chunks):
            sent = src.at[c, pl.ds(0, 16 * (n_mp - 1)), :]
            pltpu.make_async_copy(sent, sent, a_send.at[k, c]).wait()
    for k, src in enumerate((kl_v, kr_v)):
        sent = src.at[pl.ds(0, n_dp - 1)]
        pltpu.make_async_copy(sent, sent, g_send.at[k]).wait()
    store.wait()


def shards(n_dp, n_mp, tokens, right_weight, left_weight, cotangent):
    tok = tokens.shape[0]
    chunks = tok // CHUNK
    vmem, sem = pltpu.VMEM, pltpu.SemaphoreType.DMA
    any_space = pl.BlockSpec(memory_space=pl.ANY)
    in_vmem = pl.BlockSpec(memory_space=pltpu.VMEM)
    activated, grad_right, grad_left = pl.pallas_call(
        functools.partial(kernel, n_dp, n_mp),
        out_shape=[
            jax.ShapeDtypeStruct((tok, 256), BF),
            jax.ShapeDtypeStruct((4, 2, 64), F32),
            jax.ShapeDtypeStruct((4, 2, 64), F32),
        ],
        in_specs=[any_space] * 4,
        out_specs=[any_space, in_vmem, in_vmem],
        scratch_shapes=[
            vmem((tok, 256), BF),
            vmem((tok, 256), BF),
            vmem((4, 2, 64), BF),
            vmem((4, 2, 64), BF),
            vmem((256, tok), BF),
            vmem((256, tok), BF),
            vmem((chunks, 256, CHUNK), BF),
            vmem((chunks, 256, CHUNK), BF),
            vmem((chunks, 256, CHUNK), BF),
            vmem((chunks, 256, CHUNK), BF),
            vmem((256, tok), BF),
            vmem((tok, 256), BF),
            vmem((2, 256), BF),
            vmem((2, 256), BF),
            vmem((n_dp, 2, 256), BF),
            vmem((n_dp, 2, 256), BF),
            vmem((n_dp, 2, 256), F32),
            vmem((n_dp, 2, 256), F32),
            vmem((n_dp, 2, 256), F32),
            vmem((n_dp, 2, 256), F32),
            sem((4,)),
            sem,
            sem((2,)),
            sem((2,)),
            sem((2, chunks)),
            sem((2, chunks)),
            sem((2,)),
            sem((2,)),
        ],
        compiler_params=pltpu.CompilerParams(collective_id=0, has_side_effects=True),
        name="monarch",
    )(tokens, right_weight, left_weight, cotangent)
    return activated, grad_right, grad_left


def solution(mesh):
    return jax.shard_map(
        functools.partial(shards, mesh.shape["dp"], mesh.shape["mp"]),
        mesh=mesh,
        in_specs=(P("dp", "mp"), P("mp", "dp", None), P("mp", "dp", None), P("dp", "mp")),
        out_specs=(P("dp", "mp"), P("mp", "dp", None), P("mp", "dp", None)),
        check_vma=False,
    )
```

```python
import functools

import jax
import jax.numpy as jnp
from jax import lax
from jax.experimental import pallas as pl
from jax.experimental.pallas import tpu as pltpu
from jax.sharding import PartitionSpec as P

MESH = pl.DeviceIdType.MESH
BF = jnp.bfloat16
F32 = jnp.float32
CHUNK = 256
N_Z = 16
N_X = 4
NEAR = [(dz, dy) for dz in (-3, 2, -2, 1, -1, 0) for dy in (1, 0) if (dz, dy) != (0, 0)]
FAR = 5
FORWARD = [(-FAR, b) for b in (3, 2, 1, 0, -1)] + [(FAR, b) for b in (-2, -1, 0, 1, 2)]
FORWARD = [FORWARD[i + 5 * s] for i in range(5) for s in range(2)]
ALL_DP = [(dz, dy) for dz in (8, 7, -7, 6, -6, 5, -5, 4, -4, 3, -3, 2, -2, 1, -1, 0) for dy in (1, 0) if (dz, dy) != (0, 0)]
ALL_MP = [(dx, dy, dc) for dx in (2, 1, 3, 0) for dy in (1, 0) for dc in (1, 0) if (dx, dy, dc) != (0, 0, 0)]


def iota(dim, shape=(256, 256)):
    return lax.broadcasted_iota(jnp.int32, shape, dim)


def nn(a, b):
    return lax.dot_general(a, b, (((1,), (0,)), ((), ())), preferred_element_type=F32)


def nt(a, b):
    return lax.dot_general(a, b, (((1,), (1,)), ((), ())), preferred_element_type=F32)


def ones_where(cond):
    return jnp.where(cond, 1.0, 0.0).astype(BF)


def wrap(v, n):
    v = jnp.where(v >= n, v - n, v)
    return jnp.where(v < 0, v + n, v)


def diagonal_blocks(full):
    lane = iota(1, (64, 256)) // 64
    total = full[:64]
    for b in range(1, 4):
        total = jnp.where(lane == b, full[64 * b : 64 * b + 64], total)
    return total


def kernel(
    x_hbm,
    rw_hbm,
    lw_hbm,
    cot_hbm,
    act_ref,
    gr_ref,
    gl_ref,
    x_v,
    cot_v,
    rw_v,
    lw_v,
    xt_v,
    cott_v,
    s1_v,
    r_v,
    s2_v,
    d_v,
    actt_v,
    got_rw,
    got_lw,
    kr_v,
    kl_v,
    got_kr,
    got_kl,
    in_sem,
    w_send,
    w_recv,
    a_send,
    a_recv,
    g_send,
    g_recv,
):
    tok = x_v.shape[0]
    chunks = tok // CHUNK
    n_dp, n_mp = 2 * N_Z, 4 * N_X
    dp = lax.axis_index("dp")
    mp = lax.axis_index("mp")
    y = dp // N_Z
    z = dp - y * N_Z
    core = lax.rem(mp, 2)
    y_lo = lax.rem(mp // 2, 2)
    x = mp // 4

    def dp_peer(dz, dy):
        return (1 - y if dy else y) * N_Z + wrap(z + dz, N_Z)

    def mp_peer(dx, dy, dc):
        return wrap(x + dx, N_X) * 4 + (1 - y_lo if dy else y_lo) * 2 + (1 - core if dc else core)

    barrier = pltpu.get_barrier_semaphore()
    greet = [(FAR, 0), (-FAR, 0)] + [(-dz, dy) for dz, dy in NEAR]
    for dz, dy in greet:
        pl.semaphore_signal(barrier, inc=1, device_id={"dp": dp_peer(dz, dy)}, device_id_type=MESH)
    for d in ALL_MP:
        pl.semaphore_signal(barrier, inc=1, device_id={"mp": mp_peer(*d)}, device_id_type=MESH)

    loads = [
        pltpu.make_async_copy(rw_hbm, rw_v, in_sem.at[0]),
        pltpu.make_async_copy(lw_hbm, lw_v, in_sem.at[1]),
        pltpu.make_async_copy(x_hbm, x_v, in_sem.at[2]),
        pltpu.make_async_copy(cot_hbm, cot_v, in_sem.at[3]),
    ]
    for load in loads:
        load.start()

    loads[0].wait()
    loads[1].wait()
    got_rw[y, z] = jnp.concatenate([rw_v[i].astype(F32) for i in range(4)], axis=1).astype(BF)
    got_lw[y, z] = jnp.concatenate([lw_v[i].astype(F32) for i in range(4)], axis=1).astype(BF)
    loads[2].wait()
    loads[3].wait()
    xt_v[...] = x_v[...].T
    cott_v[...] = cot_v[...].T

    pl.semaphore_wait(barrier, len(greet) + len(ALL_MP))

    gathers = (got_rw, got_lw)
    for k, got in enumerate(gathers):
        for dz, dy in NEAR:
            pltpu.make_async_remote_copy(
                src_ref=got.at[y, z],
                dst_ref=got.at[y, z],
                send_sem=w_send.at[k, 0],
                recv_sem=w_recv.at[k, 0],
                device_id={"dp": dp_peer(dz, dy)},
                device_id_type=MESH,
            ).start()

    row, col = iota(0), iota(1)
    to_r = ones_where(col == (row % 4) * 64 + row // 4)
    from_r = ones_where(row == (col % 4) * 64 + col // 4)
    rep = ones_where(iota(1, (256, 64)) == (iota(0, (256, 64)) // 16) * 4 + iota(0, (256, 64)) % 4)

    def near_blocks(k):
        return gathers[k].at[0, pl.ds(0, len(NEAR))]

    def far_blocks(k):
        return gathers[k].at[:, pl.ds(0, len(FORWARD))]

    for k, got in enumerate(gathers):
        pltpu.make_async_copy(near_blocks(k), near_blocks(k), w_recv.at[k, 0]).wait()
        for dz, b in FORWARD:
            blocks = got.at[:, wrap(z + b, N_Z)]
            pltpu.make_async_remote_copy(
                src_ref=blocks,
                dst_ref=blocks,
                send_sem=w_send.at[k, 1],
                recv_sem=w_recv.at[k, 1],
                device_id={"dp": dp_peer(dz, 0)},
                device_id_type=MESH,
            ).start()

    pltpu.make_async_copy(far_blocks(0), far_blocks(0), w_recv.at[0, 1]).wait()
    rows = got_rw[...].reshape(64, 256).astype(F32)
    lane = iota(1, (64, 256)) // 64
    block_diag = jnp.concatenate([jnp.where(lane == b, rows, 0.0) for b in range(4)], axis=0).astype(BF)
    first = nt(to_r, block_diag).astype(BF)

    mine = pl.ds(pl.multiple_of(16 * mp, 16), 16)

    def exchange(c, src, dst, k):
        for d in ALL_MP:
            q = mp_peer(*d)
            pltpu.make_async_remote_copy(
                src_ref=src.at[c, pl.ds(pl.multiple_of(16 * q, 16), 16), :],
                dst_ref=dst.at[c, mine, :],
                send_sem=a_send.at[k, c],
                recv_sem=a_recv.at[k, c],
                device_id={"mp": q},
                device_id_type=MESH,
            ).start()
        dst[c, mine, :] = src[c, mine, :]

    def arrived(dst, c, k):
        others = dst.at[c, pl.ds(0, 16 * (n_mp - 1)), :]
        pltpu.make_async_copy(others, others, a_recv.at[k, c]).wait()

    for c in range(chunks):
        s1_v[c] = nn(first, xt_v[:, CHUNK * c : CHUNK * (c + 1)]).astype(BF)
        exchange(c, s1_v, r_v, 0)

    pltpu.make_async_copy(far_blocks(1), far_blocks(1), w_recv.at[1, 1]).wait()
    spread = nn(rep, got_lw[...].reshape(64, 256))
    second_f = jnp.where(col // 64 == (row // 4) % 4, spread, 0.0)
    second = second_f.astype(BF)
    second_t = second_f.T.astype(BF)

    left = jnp.zeros((256, 256), F32)
    for c in range(chunks):
        arrived(r_v, c, 0)
        inner = r_v[c]
        pre = nn(second_t, inner)
        cdf = 0.5 * (1.0 + lax.erf(pre * 0.7071067811865476))
        density = jnp.exp(-0.5 * pre * pre) * 0.3989422804014327
        cot = cott_v[:, CHUNK * c : CHUNK * (c + 1)].astype(F32)
        dpre = (cot * (cdf + pre * density)).astype(BF)
        s2_v[c] = nn(second, dpre).astype(BF)
        exchange(c, s2_v, d_v, 1)
        actt_v[:, CHUNK * c : CHUNK * (c + 1)] = (pre * cdf).astype(BF)
        left = left + nt(inner, dpre)

    def scatter(src, dst, k):
        for d in ALL_DP:
            peer = dp_peer(*d)
            pltpu.make_async_remote_copy(
                src_ref=src.at[peer],
                dst_ref=dst.at[dp],
                send_sem=g_send.at[k],
                recv_sem=g_recv.at[k],
                device_id={"dp": peer},
                device_id_type=MESH,
            ).start()
        dst[dp] = src[dp]

    def collect(dst, k):
        others = dst.at[pl.ds(0, n_dp - 1)]
        pltpu.make_async_copy(others, others, g_recv.at[k]).wait()
        return jnp.sum(dst[...], axis=0)

    left = jnp.where(col // 64 == (row // 4) % 4, left, 0.0)
    left = jnp.sum(left.reshape(16, 4, 4, 256), axis=1)
    kl_v[...] = left.reshape(n_dp, 2, 256)
    scatter(kl_v, got_kl, 0)

    right = jnp.zeros((256, 256), F32)
    for c in range(chunks):
        arrived(d_v, c, 1)
        dinner = nn(from_r, d_v[c]).astype(BF)
        right = right + nt(xt_v[:, CHUNK * c : CHUNK * (c + 1)], dinner)
    kr_v[...] = diagonal_blocks(right).reshape(n_dp, 2, 256)
    scatter(kr_v, got_kr, 1)

    act_ref[...] = actt_v[...].T

    sum_l = collect(got_kl, 0)
    for b in range(4):
        gl_ref[b] = sum_l[:, 64 * b : 64 * b + 64]
    for k in range(2):
        pltpu.make_async_copy(near_blocks(k), near_blocks(k), w_send.at[k, 0]).wait()
        pltpu.make_async_copy(far_blocks(k), far_blocks(k), w_send.at[k, 1]).wait()
    for k, src in enumerate((s1_v, s2_v)):
        for c in range(chunks):
            sent = src.at[c, pl.ds(0, 16 * (n_mp - 1)), :]
            pltpu.make_async_copy(sent, sent, a_send.at[k, c]).wait()
    for k, src in enumerate((kl_v, kr_v)):
        sent = src.at[pl.ds(0, n_dp - 1)]
        pltpu.make_async_copy(sent, sent, g_send.at[k]).wait()
    sum_r = collect(got_kr, 1)
    for b in range(4):
        gr_ref[b] = sum_r[:, 64 * b : 64 * b + 64]


def write_out(act, gr, gl, act_hbm, gr_hbm, gl_hbm, sem):
    copies = [
        pltpu.make_async_copy(src, dst, sem.at[k])
        for k, (src, dst) in enumerate(((act, act_hbm), (gr, gr_hbm), (gl, gl_hbm)))
    ]
    for copy in copies:
        copy.start()
    for copy in copies:
        copy.wait()


def shards(tokens, right_weight, left_weight, cotangent):
    tok = tokens.shape[0]
    chunks = tok // CHUNK
    n_dp = 2 * N_Z
    vmem, sem = pltpu.VMEM, pltpu.SemaphoreType.DMA
    any_space = pl.BlockSpec(memory_space=pl.ANY)
    in_vmem = pl.BlockSpec(memory_space=pltpu.VMEM)
    shapes = [((tok, 256), BF), ((4, 2, 64), F32), ((4, 2, 64), F32)]
    results = pl.pallas_call(
        kernel,
        out_shape=[pltpu.VMEM(*s) for s in shapes],
        in_specs=[any_space] * 4,
        out_specs=[in_vmem] * 3,
        scratch_shapes=[
            vmem((tok, 256), BF),
            vmem((tok, 256), BF),
            vmem((4, 2, 64), BF),
            vmem((4, 2, 64), BF),
            vmem((256, tok), BF),
            vmem((256, tok), BF),
            vmem((chunks, 256, CHUNK), BF),
            vmem((chunks, 256, CHUNK), BF),
            vmem((chunks, 256, CHUNK), BF),
            vmem((chunks, 256, CHUNK), BF),
            vmem((256, tok), BF),
            vmem((2, N_Z, 2, 256), BF),
            vmem((2, N_Z, 2, 256), BF),
            vmem((n_dp, 2, 256), F32),
            vmem((n_dp, 2, 256), F32),
            vmem((n_dp, 2, 256), F32),
            vmem((n_dp, 2, 256), F32),
            sem((4,)),
            sem((2, 2)),
            sem((2, 2)),
            sem((2, chunks)),
            sem((2, chunks)),
            sem((2,)),
            sem((2,)),
        ],
        compiler_params=pltpu.CompilerParams(collective_id=0, has_side_effects=True),
        name="monarch",
    )(tokens, right_weight, left_weight, cotangent)
    results = [pltpu.with_memory_space_constraint(r, pltpu.VMEM) for r in results]
    return pl.pallas_call(
        write_out,
        out_shape=[jax.ShapeDtypeStruct(*s) for s in shapes],
        in_specs=[in_vmem] * 3,
        out_specs=[any_space] * 3,
        scratch_shapes=[sem((3,))],
        name="write_out",
    )(*results)


def solution(mesh):
    return jax.shard_map(
        shards,
        mesh=mesh,
        in_specs=(P("dp", "mp"), P("mp", "dp", None), P("mp", "dp", None), P("dp", "mp")),
        out_specs=(P("dp", "mp"), P("mp", "dp", None), P("mp", "dp", None)),
        check_vma=False,
    )
```
